32 devices in a mesh: tm: 16 (over z, x, core), mom: 2 (over y).
Axes of the slice: x: 2, y: 2, z: 4, core: 2. Of those that a mesh axis runs over, the one named last changes fastest.
Arguments:
- fields: bfloat16 [16, 4, 2, 512, 512], P('tm', 'mom'), may hold values from -1 to 1
- mom_pairs: int32 [6, 2], P('mom'), may hold values from 0 to 3, as said below
- deltas: int32 [4], replicated, may hold values from 0 to 3, each once
Outputs:
- time_traces: float32 [16, 2, 4, 6], P('tm', None, None, 'mom')
- summed_traces: float32 [2, 4, 6], P(None, None, 'mom')
The draws below stay inside these ranges and needn't reach their ends.
Inputs may be any that keep to these rules, and one draw needn't show every extreme that they name: `mom_pairs`: column 0 may be any momentum; in row r, column 1 lies in momentum group r // 3, that is from (r // 3) * 2 to (r // 3) * 2 + 1.
All inputs are finite; a program needn't handle non-finite values.
Results may differ from the reference program's by a relative error of at most 0.0003.
Values may be sent and summed in bfloat16 or wider, within the bound.
A program may use at most 128 MiB of HBM per device.

```python
import jax
import jax.numpy as jnp
from jax import lax

NEV = 512
PG = 2
PAIR_DEV = 3
NSEP = 4
P_SIZE = 4
NPAIR = 6
NT = 16


def draw_fields(key, part):
    field_shape = (NT, P_SIZE, 2, NEV, NEV)
    key_base = jax.random.fold_in(jax.random.fold_in(key, 11), 0)
    growth = jnp.sqrt(3.0) ** (jnp.arange(NT, dtype=jnp.float32) / max(NT - 1, 1))
    values = jax.random.normal(key_base, field_shape, jnp.float32)
    values = values * growth[:, None, None, None, None] / jnp.sqrt(jnp.float32(NEV))
    return jnp.clip(values, -1.0, 1.0).astype(jnp.bfloat16)


def draw_mom_pairs(key, part):
    key_source, key_target = jax.random.split(jax.random.fold_in(key, 23), 2)
    source_mom = jax.random.randint(key_source, (NPAIR,), 0, P_SIZE)
    owner = jnp.arange(NPAIR, dtype=jnp.int32) // PAIR_DEV
    target_mom = owner * PG + jax.random.randint(key_target, (NPAIR,), 0, PG)
    return jnp.stack([source_mom, target_mom], axis=1).astype(jnp.int32)


def setup_inputs(seed: int = 0) -> dict:
    streams_of = jax.random.split(jax.random.key(seed), 4)
    fields = draw_fields(jax.random.fold_in(streams_of[3], 71), 0)
    mom_pairs = draw_mom_pairs(jax.random.fold_in(streams_of[3], 71), 0)
    deltas = jax.random.permutation(streams_of[2], NSEP).astype(jnp.int32)
    return dict(fields=fields, mom_pairs=mom_pairs, deltas=deltas)


def products(source, target):
    product_full = jnp.einsum("xij,yjk->xyik", source.astype(jnp.float32), target.astype(jnp.float32))
    real_part = product_full[0, 0] - product_full[1, 1]
    imag_part = product_full[0, 1] + product_full[1, 0]
    direct = jnp.trace(real_part)
    box_value = jnp.sum(real_part * real_part.T) - jnp.sum(imag_part * imag_part.T)
    return direct, box_value


def reference(fields, mom_pairs, deltas):
    slices = fields.shape[0]
    pair_count = mom_pairs.shape[0]

    def one_time(time_slice):
        source_slice = lax.dynamic_index_in_dim(fields, time_slice, 0, keepdims=False)
        per_sep = []
        for separation in range(1, NSEP + 1):
            later = ((time_slice + separation) % slices).astype(jnp.int32)
            target_slice = lax.dynamic_index_in_dim(fields, later, 0, keepdims=False)
            directs = []
            boxes = []
            for which in range(pair_count):
                source = lax.dynamic_index_in_dim(source_slice, mom_pairs[which, 0].astype(jnp.int32), 0, keepdims=False)
                target = lax.dynamic_index_in_dim(target_slice, mom_pairs[which, 1].astype(jnp.int32), 0, keepdims=False)
                direct, box_value = products(source, target)
                directs.append(direct)
                boxes.append(box_value)
            per_sep.append(jnp.stack([jnp.stack(directs), jnp.stack(boxes)]))
        return jnp.stack(per_sep, axis=1)

    stacked = lax.map(one_time, jnp.arange(slices, dtype=jnp.int32))
    time_traces = jnp.take(stacked, deltas.astype(jnp.int32), axis=2)
    summed_traces = jnp.sum(time_traces, axis=0)
    return time_traces, summed_traces
```

```python
import functools

import jax
import jax.numpy as jnp
from jax import lax
from jax.experimental import pallas as pl
from jax.experimental.pallas import tpu as pltpu
from jax.sharding import PartitionSpec as P

MESH = pl.DeviceIdType.MESH
BLK = 128
ROWS = 64
LAG = 3
EARLY = 1


def kernel(n_tm, n_mom, pair_ref, delta_ref, field_ref, out_ref, *scratch):
    per_group, _, nev, _ = field_ref.shape[1:]
    stages = nev // BLK
    slots = 4
    pairs = pair_ref.shape[1]
    seps = delta_ref.shape[0]
    halves = BLK // ROWS
    parts = per_group * 2
    groups = stages * halves
    steps = groups * parts
    columns = n_tm // 4
    a_bufs = scratch[:stages]
    banks = [scratch[stages + q * groups : stages + (q + 1) * groups] for q in range(slots + 1)]
    b_bufs, own = banks[:slots], banks[slots]
    early, acc_d, acc_b, held, gathered = scratch[stages + (slots + 1) * groups :][:5]
    (own_sem, left_sem, y_send, y_recv, far_send, far_recv, b_send, b_recv, e_send, e_recv, f_send, r_send, r_recv,
     chain, rounds) = scratch[-15:]

    me = lax.axis_index("tm")
    group = lax.axis_index("mom")
    core = lax.rem(me, 2)
    upper_core = core == 1
    lower_core = core == 0
    odd_chip = lax.rem(me // 2, 2) == 1
    even_chip = lax.rem(me // 2, 2) == 0
    level = me // 4
    first_level = level == 0
    last_level = level == columns - 1

    def at(step):
        return {"tm": lax.rem(me + step + n_tm, n_tm), "mom": group}

    beside = {"tm": me + 2 - 4 * lax.rem(me // 2, 2), "mom": group}
    twin = {"tm": me + 1 - 2 * core, "mom": group}
    below = at(-4)
    above = at(4)
    across_from = [{"tm": me, "mom": lax.rem(group + j, n_mom)} for j in range(1, n_mom)]

    barrier = pltpu.get_barrier_semaphore()

    def greet(device):
        pl.semaphore_signal(barrier, inc=1, device_id=device, device_id_type=MESH)

    @pl.when(jnp.logical_not(first_level))
    def _():
        greet(below)

    @pl.when(jnp.logical_not(last_level))
    def _():
        greet(above)

    for device in [beside, twin] + across_from:
        greet(device)

    def load_own(g):
        return pltpu.make_async_copy(field_ref.at[0, :, :, pl.ds(g * ROWS, ROWS), :], own[g], own_sem.at[g])

    def load_left(n):
        return pltpu.make_async_copy(
            field_ref.at[0, :, :, :, pl.ds(n * BLK, BLK)],
            a_bufs[n].at[pl.ds(group * per_group, per_group)],
            left_sem.at[n],
        )

    for g in range(groups):
        load_own(g).start()
    for n in range(stages):
        load_left(n).start()
    for g in range(groups):
        load_own(g).wait()

    ends = jnp.where(first_level, 1, 0) + jnp.where(last_level, 1, 0)
    pl.semaphore_wait(barrier, n_mom + 3 - ends)

    def pass_chain():
        pl.semaphore_signal(chain, inc=1, device_id=below, device_id_type=MESH)

    if columns > 2:
        pl.when(level == columns - 2)(pass_chain)

    def piece(buf, i):
        g, rest = divmod(i, parts)
        return buf[g].at[rest // 2, rest % 2]

    def far(i, src):
        return pltpu.make_async_remote_copy(
            src_ref=piece(src, i),
            dst_ref=piece(b_bufs[0], i),
            send_sem=far_send.at[i],
            recv_sem=far_recv.at[i],
            device_id=below,
            device_id_type=MESH,
        )

    def near(q, g, src):
        return pltpu.make_async_remote_copy(
            src_ref=src[g],
            dst_ref=b_bufs[q][g],
            send_sem=b_send.at[q - 1, g],
            recv_sem=b_recv.at[q - 1, g],
            device_id=beside if q == 1 else twin,
            device_id_type=MESH,
        )

    def near_piece(i, src):
        return pltpu.make_async_remote_copy(
            src_ref=piece(src, i),
            dst_ref=piece(b_bufs[1], i),
            send_sem=b_send.at[0, i // parts],
            recv_sem=b_recv.at[0, i // parts],
            device_id=beside,
            device_id_type=MESH,
        )

    detour = range(steps - EARLY, steps)

    def give_early(i):
        return pltpu.make_async_remote_copy(
            src_ref=piece(own, i),
            dst_ref=early.at[i - detour[0]],
            send_sem=e_send.at[i - detour[0]],
            recv_sem=e_recv.at[i - detour[0]],
            device_id=beside,
            device_id_type=MESH,
        )

    def pass_early(i):
        return pltpu.make_async_remote_copy(
            src_ref=early.at[i - detour[0]],
            dst_ref=piece(b_bufs[1], i),
            send_sem=f_send.at[i - detour[0]],
            recv_sem=b_recv.at[0, i // parts],
            device_id=below,
            device_id_type=MESH,
        )

    def across(n, j):
        part = a_bufs[n].at[pl.ds(group * per_group, per_group)]
        return pltpu.make_async_remote_copy(
            src_ref=part,
            dst_ref=part,
            send_sem=y_send.at[n, j],
            recv_sem=y_recv.at[n, j],
            device_id=across_from[j],
            device_id_type=MESH,
        )

    def send_far(some):
        for i in some:
            far(i, own).start()

    if EARLY:

        @pl.when(even_chip)
        def _():
            for i in detour:
                give_early(i).start()

    for n in range(stages):
        @pl.when(jnp.logical_not(first_level))
        def _():
            send_far(range(n * halves * parts, (n + 1) * halves * parts))

        load_left(n).wait()
        for j in range(n_mom - 1):
            across(n, j).start()

        @pl.when(odd_chip)
        def _():
            for g in range(n * halves, (n + 1) * halves):
                near(1, g, own).start()

        @pl.when(upper_core)
        def _():
            for g in range(n * halves, (n + 1) * halves):
                near(2, g, own).start()

    if columns > 2:

        @pl.when(jnp.logical_and(level < columns - 2, jnp.logical_not(first_level)))
        def _():
            pl.semaphore_wait(chain, 1)
            pass_chain()

        @pl.when(first_level)
        def _():
            pl.semaphore_wait(chain, 1)

    @pl.when(first_level)
    def _():
        send_far(range(steps))

    if EARLY:

        @pl.when(odd_chip)
        def _():
            for i in detour:
                give_early(i).wait_recv()
                pass_early(i).start()

    def pass_far(i):
        far(i, b_bufs[0]).wait_recv()
        if i not in detour:

            @pl.when(even_chip)
            def _():
                near_piece(i, b_bufs[0]).start()

        if i % parts == parts - 1:

            @pl.when(lower_core)
            def _():
                near(2, i // parts, b_bufs[0]).start()

    def pass_near(g):
        near(1, g, b_bufs[1]).wait_recv()
        near(3, g, b_bufs[1]).start()

    def meet(r, devices):
        for device in devices:
            pl.semaphore_signal(rounds.at[r], inc=1, device_id=device, device_id_type=MESH)
        pl.semaphore_wait(rounds.at[r], len(devices))

    reach = 4
    meetings = []
    while 2 * reach < n_tm:
        meetings.append([at(-reach), at(reach)])
        reach *= 2
    meetings += [[beside], [twin]]

    acc_d[...] = jnp.zeros_like(acc_d)
    acc_b[...] = jnp.zeros_like(acc_b)
    eye = (
        lax.broadcasted_iota(jnp.int32, (BLK, BLK), 0) == lax.broadcasted_iota(jnp.int32, (BLK, BLK), 1)
    ).astype(jnp.float32)

    def fold(x):
        return jnp.sum(x.reshape(x.shape[0] // 8, 8, BLK), axis=0)

    def weight(n, k):
        a = pair_ref[0, k]
        re, im = a_bufs[n][a, 0], a_bufs[n][a, 1]
        return jnp.concatenate(
            [jnp.concatenate([re, im], axis=1), jnp.concatenate([-im, re], axis=1)], axis=0
        )

    def rows(q, some, k):
        b = lax.rem(pair_ref[1, k], per_group)
        return jnp.concatenate(
            [jnp.concatenate([b_bufs[q][g][b, 0], b_bufs[q][g][b, 1]], axis=1) for g in some], axis=0
        )

    def columns_of(n, k):
        product = jnp.dot(
            jnp.concatenate([rows(q, range(n * halves), k) for q in range(slots)], axis=0),
            weight(n, k),
            preferred_element_type=jnp.float32,
        )
        for q in range(slots):
            for m in range(n):
                block = product[(q * n + m) * BLK : (q * n + m + 1) * BLK]
                held[q * pairs + k, m, 0] = block[:, :BLK].T
                held[q * pairs + k, m, 1] = block[:, BLK:].T

    def rows_of(n, qs, k, part=None):
        some = range(halves) if part is None else [part]
        begin, size = some[0] * ROWS, len(some) * ROWS
        lhs = jnp.concatenate([rows(q, [n * halves + h for h in some], k) for q in qs], axis=0)
        span = pl.ds(begin, size)
        box = [None] * len(qs)
        for m in range(n, -1, -1):
            product = jnp.dot(lhs, weight(m, k), preferred_element_type=jnp.float32)
            for p, q in enumerate(qs):
                index = q * pairs + k
                re, im = product[p * size : (p + 1) * size, :BLK], product[p * size : (p + 1) * size, BLK:]
                if m < n:
                    box[p] += fold(re * held[index, m, 0, span] - im * held[index, m, 1, span])
                    continue
                box[p] = jnp.zeros((8, BLK), jnp.float32)
                if begin + size < BLK:
                    held[index, n, 0, span] = re
                    held[index, n, 1, span] = im
                    continue
                if begin:
                    re = jnp.concatenate([held[index, n, 0, pl.ds(0, begin)], re], axis=0)
                    im = jnp.concatenate([held[index, n, 1, pl.ds(0, begin)], im], axis=0)
                acc_d[index] += fold(re * eye)
                acc_b[index] += fold(re * re.T - im * im.T)
        if n:
            for p, q in enumerate(qs):
                acc_b[q * pairs + k] += box[p] + box[p]

    def lefts(n):
        for j in range(n_mom - 1):
            across(n, j).wait_recv()

    def work(n, j):
        if j == 0:
            lefts(n)
        if n:
            for k in range(pairs)[j::3] if j < 3 else ():
                columns_of(n, k)
        if j == 3:
            for g in range(n * halves, (n + 1) * halves):
                near(2, g, b_bufs[2]).wait_recv()
            rows_of(n, (0, 2), 0)
        if j == 4:
            for k in range(1, pairs):
                rows_of(n, (0, 2), k)
        if j == 5:
            for g in range(n * halves, (n + 1) * halves):
                near(3, g, b_bufs[3]).wait_recv()
            rows_of(n, (1, 3), 0)
        if j == 6:
            for k in range(1, pairs):
                rows_of(n, (1, 3), k)

    per_stage = halves * parts
    for i in range(steps):
        pass_far(i)
        g, rest = divmod(i - LAG, parts)
        if g >= 0 and rest == parts - 1:
            pass_near(g)
        if i % 4 == 1 and i // 4 < len(meetings):
            meet(i // 4, meetings[i // 4])
        if i >= per_stage:
            work(i // per_stage - 1, i % per_stage)
    last = stages - 1
    lefts(last)
    for k in range(pairs):
        columns_of(last, k)
    for h in range(halves):
        g = last * halves + h
        near(2, g, b_bufs[2]).wait_recv()
        if h == halves - 1:
            pass_near(g)
        for k in range(pairs):
            rows_of(last, (0, 2), k, h)
        near(3, g, b_bufs[3]).wait_recv()
        for k in range(pairs):
            rows_of(last, (1, 3), k, h)

    count = acc_d.shape[0]
    height = gathered.shape[1]
    lane = lax.broadcasted_iota(jnp.int32, (1, BLK), 1)
    wanted = jnp.zeros((1, BLK), jnp.int32)
    for r in range(seps):
        wanted = jnp.where(lane == r, delta_ref[r], wanted)
    place = jnp.where(wanted == 0, 2 + core, jnp.where(wanted == 1, 1, jnp.where(wanted == 2, 3 - core, 0)))
    index = lax.broadcasted_iota(jnp.int32, (count, BLK), 0)
    which = lax.broadcasted_iota(jnp.int32, (height, BLK), 0)
    stat = jnp.zeros((height, BLK), jnp.float32)
    for p, acc in enumerate((acc_d, acc_b)):
        each = jnp.sum(jnp.sum(acc[...], axis=1), axis=1, keepdims=True)
        each = jnp.broadcast_to(each, (count, BLK))
        for k in range(pairs):
            line = jnp.sum(jnp.where(index == place * pairs + k, each, 0.0), axis=0, keepdims=True)
            stat = jnp.where(which == 2 * k + p, jnp.broadcast_to(line, (height, BLK)), stat)
    gathered[me] = stat

    def give(i):
        return pltpu.make_async_remote_copy(
            src_ref=gathered.at[me],
            dst_ref=gathered.at[me],
            send_sem=r_send.at[i],
            recv_sem=r_recv.at[i],
            device_id=at(i),
            device_id_type=MESH,
        )

    order = sorted(range(1, n_tm), key=lambda i: -min(i, n_tm - i))
    for i in order:
        give(i).start()
    out_ref[0] = stat
    for n in range(stages):
        for j in range(n_mom - 1):
            across(n, j).wait_send()
    for i in range(steps):
        far(i, own).wait_send()
    for g in range(groups):
        for q in range(2, slots):
            near(q, g, own).wait_send()

    @pl.when(odd_chip)
    def _():
        for g in range(groups):
            near(1, g, own).wait_send()
        for i in detour:
            pass_early(i).wait_send()

    @pl.when(even_chip)
    def _():
        for g in range(groups):
            kept = [i for i in range(g * parts, (g + 1) * parts) if i not in detour]
            if len(kept) == parts:
                near(1, g, own).wait_send()
            else:
                for i in kept:
                    near_piece(i, own).wait_send()
        for i in detour:
            give_early(i).wait_send()

    for i in reversed(order):
        give(i).wait()
    out_ref[1] = jnp.sum(gathered[...], axis=0)


def split(stat_ref, local_ref, sum_ref):
    pairs, _, seps = local_ref.shape
    for ref, place in ((local_ref, 0), (sum_ref, 1)):
        for k in range(pairs):
            ref[k] = stat_ref[place, 2 * k : 2 * k + 2, :seps]


def per_device(n_tm, n_mom, fields, mom_pairs, deltas):
    _, per_group, _, nev, _ = fields.shape
    pairs = mom_pairs.shape[0]
    seps = deltas.shape[0]
    stages = nev // BLK
    slots = 4
    groups = nev // ROWS
    steps = groups * per_group * 2
    meetings = 2
    reach = 4
    while 2 * reach < n_tm:
        meetings += 1
        reach *= 2
    count = -(-slots * pairs // 8) * 8
    height = -(-2 * pairs // 8) * 8
    dma = pltpu.SemaphoreType.DMA
    scratch = (
        [pltpu.VMEM((n_mom * per_group, 2, nev, BLK), fields.dtype)] * stages
        + [pltpu.VMEM((per_group, 2, ROWS, nev), fields.dtype)] * (groups * (slots + 1))
        + [pltpu.VMEM((max(EARLY, 1), ROWS, nev), fields.dtype)]
        + [pltpu.VMEM((count, 8, BLK), jnp.float32)] * 2
        + [pltpu.VMEM((count, stages, 2, BLK, BLK), jnp.float32)]
        + [pltpu.VMEM((n_tm, height, BLK), jnp.float32)]
        + [dma((groups,)), dma((stages,))]
        + [dma((stages, n_mom))] * 2
        + [dma((steps,))] * 2
        + [dma((slots - 1, groups))] * 2
        + [dma((max(EARLY, 1),))] * 3
        + [dma((n_tm,))] * 2
        + [pltpu.SemaphoreType.REGULAR, pltpu.SemaphoreType.REGULAR((meetings,))]
    )
    stat = pl.pallas_call(
        functools.partial(kernel, n_tm, n_mom),
        out_shape=jax.ShapeDtypeStruct((2, height, BLK), jnp.float32),
        in_specs=[
            pl.BlockSpec(memory_space=pltpu.SMEM),
            pl.BlockSpec(memory_space=pltpu.SMEM),
            pl.BlockSpec(memory_space=pltpu.HBM),
        ],
        out_specs=pl.BlockSpec(memory_space=pltpu.VMEM),
        scratch_shapes=scratch,
        compiler_params=pltpu.CompilerParams(
            collective_id=0, has_side_effects=True, vmem_limit_bytes=67_043_328
        ),
    )(mom_pairs.T, deltas, fields)
    tile = jax.ShapeDtypeStruct((pairs, 2, seps), jnp.float32)
    local, total = pl.pallas_call(
        split,
        out_shape=(tile, tile),
        in_specs=[pl.BlockSpec(memory_space=pltpu.VMEM)],
        out_specs=(pl.BlockSpec(memory_space=pltpu.VMEM), pl.BlockSpec(memory_space=pltpu.VMEM)),
    )(stat)
    return (local.transpose(1, 2, 0)[None], total.transpose(1, 2, 0))


def solution(mesh):
    return jax.shard_map(
        functools.partial(per_device, mesh.shape["tm"], mesh.shape["mom"]),
        mesh=mesh,
        in_specs=(P("tm", "mom", None, None, None), P("mom", None), P()),
        out_specs=(P("tm", None, None, "mom"), P(None, None, "mom")),
        check_vma=False,
    )
```

```python
import functools

import jax
import jax.numpy as jnp
from jax import lax
from jax.experimental import pallas as pl
from jax.experimental.pallas import tpu as pltpu
from jax.sharding import PartitionSpec as P

MESH = pl.DeviceIdType.MESH
BLK = 128
ROWS = 64
LAG = 3
EARLY = 1


def kernel(n_tm, n_mom, pair_ref, delta_ref, field_ref, out_ref, *scratch):
    per_group, _, nev, _ = field_ref.shape[1:]
    stages = nev // BLK
    slots = 4
    pairs = pair_ref.shape[1]
    seps = delta_ref.shape[0]
    halves = BLK // ROWS
    parts = per_group * 2
    groups = stages * halves
    steps = groups * parts
    columns = n_tm // 4
    a_bufs = scratch[:stages]
    banks = [scratch[stages + q * groups : stages + (q + 1) * groups] for q in range(slots + 1)]
    b_bufs, own = banks[:slots], banks[slots]
    early, acc_d, acc_b, held, kept_rows, gathered = scratch[stages + (slots + 1) * groups :][:6]
    (own_sem, left_sem, y_send, y_recv, far_send, far_recv, b_send, b_recv, e_send, e_recv, f_send, r_send, r_recv,
     chain, rounds) = scratch[-15:]

    me = lax.axis_index("tm")
    group = lax.axis_index("mom")
    core = lax.rem(me, 2)
    upper_core = core == 1
    lower_core = core == 0
    odd_chip = lax.rem(me // 2, 2) == 1
    even_chip = lax.rem(me // 2, 2) == 0
    level = me // 4
    first_level = level == 0
    last_level = level == columns - 1

    def at(step):
        return {"tm": lax.rem(me + step + n_tm, n_tm), "mom": group}

    beside = {"tm": me + 2 - 4 * lax.rem(me // 2, 2), "mom": group}
    twin = {"tm": me + 1 - 2 * core, "mom": group}
    below = at(-4)
    above = at(4)
    across_from = [{"tm": me, "mom": lax.rem(group + j, n_mom)} for j in range(1, n_mom)]

    barrier = pltpu.get_barrier_semaphore()

    def greet(device):
        pl.semaphore_signal(barrier, inc=1, device_id=device, device_id_type=MESH)

    @pl.when(jnp.logical_not(first_level))
    def _():
        greet(below)

    @pl.when(jnp.logical_not(last_level))
    def _():
        greet(above)

    for device in [beside, twin] + across_from:
        greet(device)

    def load_own(g):
        return pltpu.make_async_copy(field_ref.at[0, :, :, pl.ds(g * ROWS, ROWS), :], own[g], own_sem.at[g])

    def load_left(n):
        return pltpu.make_async_copy(
            field_ref.at[0, :, :, :, pl.ds(n * BLK, BLK)],
            a_bufs[n].at[pl.ds(group * per_group, per_group)],
            left_sem.at[n],
        )

    for n in range(stages):
        for g in range(n * halves, (n + 1) * halves):
            load_own(g).start()
        load_left(n).start()

    ends = jnp.where(first_level, 1, 0) + jnp.where(last_level, 1, 0)
    pl.semaphore_wait(barrier, n_mom + 3 - ends)

    def pass_chain():
        pl.semaphore_signal(chain, inc=1, device_id=below, device_id_type=MESH)

    if columns > 2:
        pl.when(level == columns - 2)(pass_chain)

    def piece(buf, i):
        g, rest = divmod(i, parts)
        return buf[g].at[rest // 2, rest % 2]

    def far(i, src):
        return pltpu.make_async_remote_copy(
            src_ref=piece(src, i),
            dst_ref=piece(b_bufs[0], i),
            send_sem=far_send.at[i],
            recv_sem=far_recv.at[i],
            device_id=below,
            device_id_type=MESH,
        )

    def near(q, g, src):
        return pltpu.make_async_remote_copy(
            src_ref=src[g],
            dst_ref=b_bufs[q][g],
            send_sem=b_send.at[q - 1, g],
            recv_sem=b_recv.at[q - 1, g],
            device_id=beside if q == 1 else twin,
            device_id_type=MESH,
        )

    def near_piece(i, src):
        return pltpu.make_async_remote_copy(
            src_ref=piece(src, i),
            dst_ref=piece(b_bufs[1], i),
            send_sem=b_send.at[0, i // parts],
            recv_sem=b_recv.at[0, i // parts],
            device_id=beside,
            device_id_type=MESH,
        )

    detour = range(steps - EARLY, steps)

    def give_early(i):
        return pltpu.make_async_remote_copy(
            src_ref=piece(own, i),
            dst_ref=early.at[i - detour[0]],
            send_sem=e_send.at[i - detour[0]],
            recv_sem=e_recv.at[i - detour[0]],
            device_id=beside,
            device_id_type=MESH,
        )

    def pass_early(i):
        return pltpu.make_async_remote_copy(
            src_ref=early.at[i - detour[0]],
            dst_ref=piece(b_bufs[1], i),
            send_sem=f_send.at[i - detour[0]],
            recv_sem=b_recv.at[0, i // parts],
            device_id=below,
            device_id_type=MESH,
        )

    def across(n, j):
        part = a_bufs[n].at[pl.ds(group * per_group, per_group)]
        return pltpu.make_async_remote_copy(
            src_ref=part,
            dst_ref=part,
            send_sem=y_send.at[n, j],
            recv_sem=y_recv.at[n, j],
            device_id=across_from[j],
            device_id_type=MESH,
        )

    def send_far(some):
        for i in some:
            far(i, own).start()

    if EARLY:

        for g in range(detour[0] // parts, groups):
            load_own(g).wait()

        @pl.when(even_chip)
        def _():
            for i in detour:
                give_early(i).start()

    for n in range(stages):
        for g in range(n * halves, (n + 1) * halves):
            if g * parts + parts <= detour[0]:
                load_own(g).wait()

        @pl.when(jnp.logical_not(first_level))
        def _():
            send_far(range(n * halves * parts, (n + 1) * halves * parts))

        load_left(n).wait()
        for j in range(n_mom - 1):
            across(n, j).start()

        @pl.when(odd_chip)
        def _():
            for g in range(n * halves, (n + 1) * halves):
                near(1, g, own).start()

        @pl.when(upper_core)
        def _():
            for g in range(n * halves, (n + 1) * halves):
                near(2, g, own).start()

    if columns > 2:

        @pl.when(jnp.logical_and(level < columns - 2, jnp.logical_not(first_level)))
        def _():
            pl.semaphore_wait(chain, 1)
            pass_chain()

        @pl.when(first_level)
        def _():
            pl.semaphore_wait(chain, 1)

    @pl.when(first_level)
    def _():
        send_far(range(steps))

    if EARLY:

        @pl.when(odd_chip)
        def _():
            for i in detour:
                give_early(i).wait_recv()
                pass_early(i).start()

    def pass_far(i):
        far(i, b_bufs[0]).wait_recv()
        if i not in detour:

            @pl.when(even_chip)
            def _():
                near_piece(i, b_bufs[0]).start()

        if i % parts == parts - 1:

            @pl.when(lower_core)
            def _():
                near(2, i // parts, b_bufs[0]).start()

    def pass_near(g):
        near(1, g, b_bufs[1]).wait_recv()
        near(3, g, b_bufs[1]).start()

    def meet(r):
        if r:
            pl.semaphore_wait(rounds.at[r - 1], len(meetings[r - 1]))
        for device in meetings[r] if r < len(meetings) else ():
            pl.semaphore_signal(rounds.at[r], inc=1, device_id=device, device_id_type=MESH)

    reach = 4
    meetings = []
    while 2 * reach < n_tm:
        meetings.append([at(-reach), at(reach)])
        reach *= 2
    meetings += [[beside], [twin]]

    acc_d[...] = jnp.zeros_like(acc_d)
    acc_b[...] = jnp.zeros_like(acc_b)
    eye = (
        lax.broadcasted_iota(jnp.int32, (BLK, BLK), 0) == lax.broadcasted_iota(jnp.int32, (BLK, BLK), 1)
    ).astype(jnp.float32)

    def fold(x):
        return jnp.sum(x.reshape(x.shape[0] // 8, 8, BLK), axis=0)

    def weight(n, k):
        a = pair_ref[0, k]
        re, im = a_bufs[n][a, 0], a_bufs[n][a, 1]
        return jnp.concatenate(
            [jnp.concatenate([re, im], axis=1), jnp.concatenate([-im, re], axis=1)], axis=0
        )

    def rows(q, some, k):
        b = lax.rem(pair_ref[1, k], per_group)
        return jnp.concatenate(
            [jnp.concatenate([b_bufs[q][g][b, 0], b_bufs[q][g][b, 1]], axis=1) for g in some], axis=0
        )

    def columns_of(n, k, kept=()):
        product = jnp.dot(
            jnp.concatenate([rows(q, range(n * halves), k) for q in range(slots)], axis=0),
            weight(n, k),
            preferred_element_type=jnp.float32,
        )
        for q in range(slots):
            for m in range(n):
                block = product[(q * n + m) * BLK : (q * n + m + 1) * BLK]
                index = q * pairs + k
                re, im = block[:, :BLK].T, block[:, BLK:].T
                held[index, m, 0] = re
                held[index, m, 1] = im
                if q in kept:
                    box = fold(kept_rows[index, m, 0] * re[:ROWS] - kept_rows[index, m, 1] * im[:ROWS])
                    acc_b[index] += box + box

    def keep_rows(n, qs, k):
        lhs = jnp.concatenate([rows(q, [n * halves], k) for q in qs], axis=0)
        for m in range(n):
            product = jnp.dot(lhs, weight(m, k), preferred_element_type=jnp.float32)
            for p, q in enumerate(qs):
                kept_rows[q * pairs + k, m, 0] = product[p * ROWS : (p + 1) * ROWS, :BLK]
                kept_rows[q * pairs + k, m, 1] = product[p * ROWS : (p + 1) * ROWS, BLK:]

    def rows_of(n, qs, k, part=None, lowest=0):
        some = range(halves) if part is None else [part]
        begin, size = some[0] * ROWS, len(some) * ROWS
        lhs = jnp.concatenate([rows(q, [n * halves + h for h in some], k) for q in qs], axis=0)
        span = pl.ds(begin, size)
        box = [None] * len(qs)
        for m in range(n, lowest - 1, -1):
            product = jnp.dot(lhs, weight(m, k), preferred_element_type=jnp.float32)
            for p, q in enumerate(qs):
                index = q * pairs + k
                re, im = product[p * size : (p + 1) * size, :BLK], product[p * size : (p + 1) * size, BLK:]
                if m < n:
                    box[p] += fold(re * held[index, m, 0, span] - im * held[index, m, 1, span])
                    continue
                box[p] = jnp.zeros((8, BLK), jnp.float32)
                if begin + size < BLK:
                    held[index, n, 0, span] = re
                    held[index, n, 1, span] = im
                    continue
                if begin:
                    re = jnp.concatenate([held[index, n, 0, pl.ds(0, begin)], re], axis=0)
                    im = jnp.concatenate([held[index, n, 1, pl.ds(0, begin)], im], axis=0)
                acc_d[index] += fold(re * eye)
                acc_b[index] += fold(re * re.T - im * im.T)
        if lowest < n:
            for p, q in enumerate(qs):
                acc_b[q * pairs + k] += box[p] + box[p]

    def lefts(n):
        for j in range(n_mom - 1):
            across(n, j).wait_recv()

    def columns_all(n, ks=None, kept=()):
        if n:
            for k in range(pairs) if ks is None else ks:
                columns_of(n, k, kept)

    def rows_all(n, qs, part=None, ks=None):
        for k in range(pairs) if ks is None else ks:
            rows_of(n, qs, k, part)

    def twins(q, some):
        for g in some:
            near(q, g, b_bufs[q]).wait_recv()

    def of(n):
        return range(n * halves, (n + 1) * halves)

    def step(i):
        pass_far(i)
        g, rest = divmod(i - LAG, parts)
        if g >= 0 and rest == parts - 1:
            pass_near(g)
        r, rest = divmod(i - 1, pace)
        if i and rest == 0 and r <= len(meetings):
            meet(r)

    def plain(n):
        first, second = range(0, (pairs + 1) // 2), range((pairs + 1) // 2, pairs)
        return [
            lambda: (lefts(n), columns_all(n, [0])),
            lambda: columns_all(n, first[1:]),
            lambda: columns_all(n, second),
            lambda: (twins(2, of(n)), rows_all(n, (0, 2), None, [0])),
            lambda: rows_all(n, (0, 2), None, range(1, pairs)),
            lambda: (twins(3, of(n)), rows_all(n, (1, 3), None, [0])),
            lambda: rows_all(n, (1, 3), None, range(1, pairs)),
        ]

    per_stage = halves * parts
    last = stages - 1
    pace = min(6, (steps - 2) // len(meetings))
    for i in range(per_stage * last):
        step(i)
        if i >= per_stage:
            units = plain(i // per_stage - 1)
            if i % per_stage < len(units):
                units[i % per_stage]()

    @pl.when(jnp.logical_not(last_level))
    def _():
        n = last - 1
        units = [
            lambda: (lefts(n), columns_all(n, [0])),
            lambda: columns_all(n, range(1, pairs)),
            lambda: (twins(2, of(n)), rows_all(n, (0, 2), None, range(pairs - 1))),
            lambda: (rows_all(n, (0, 2), None, [pairs - 1]), twins(3, of(n)), rows_all(n, (1, 3), None, [0])),
            lambda: rows_all(n, (1, 3), None, range(1, pairs)),
            lambda: (twins(2, of(last)[:1]), [keep_rows(last, (0, 2), k) for k in range(pairs)]),
        ]
        for j in range(per_stage):
            step(per_stage * last + j)
            if j < len(units):
                units[j]()
        twins(3, of(last)[:1])
        for k in range(pairs):
            keep_rows(last, (1, 3), k)
        lefts(last)
        columns_all(last, kept=range(slots))
        for k in range(pairs):
            rows_of(last, range(slots), k, 0, last)
        g = groups - 1
        twins(2, [g])
        pass_near(g)
        rows_all(last, (0, 2), halves - 1)
        twins(3, [g])
        rows_all(last, (1, 3), halves - 1)

    @pl.when(last_level)
    def _():
        begin = per_stage * last
        n = last - 1
        units = [
            lambda: (lefts(n), columns_all(n)),
            lambda: (twins(2, of(n)), rows_all(n, (0, 2), None, range(pairs - 1))),
            lambda: rows_all(n, (0, 2), None, range(pairs - 1, pairs)),
            lambda: (twins(3, of(n)), rows_all(n, (1, 3))),
            lambda: (twins(2, of(last)[:1]), [keep_rows(last, (0, 2), k) for k in range(pairs)]),
            lambda: (lefts(last), columns_all(last, [0], (0, 2))),
            lambda: (
                columns_all(last, range(1, pairs), (0, 2)),
                [rows_of(last, (0, 2), k, 0, last) for k in range(pairs)],
                twins(3, of(last)[:1]),
                rows_all(last, (1, 3), 0),
            ),
        ]
        for j in range(per_stage):
            step(begin + j)
            if j < len(units):
                units[j]()
        g = groups - 1
        twins(2, [g])
        pass_near(g)
        rows_all(last, (0, 2), halves - 1)
        twins(3, [g])
        rows_all(last, (1, 3), halves - 1)

    count = acc_d.shape[0]
    height = gathered.shape[1]
    lane = lax.broadcasted_iota(jnp.int32, (1, BLK), 1)
    wanted = jnp.zeros((1, BLK), jnp.int32)
    for r in range(seps):
        wanted = jnp.where(lane == r, delta_ref[r], wanted)
    place = jnp.where(wanted == 0, 2 + core, jnp.where(wanted == 1, 1, jnp.where(wanted == 2, 3 - core, 0)))
    index = lax.broadcasted_iota(jnp.int32, (count, BLK), 0)
    which = lax.broadcasted_iota(jnp.int32, (height, BLK), 0)
    stat = jnp.zeros((height, BLK), jnp.float32)
    for p, acc in enumerate((acc_d, acc_b)):
        each = jnp.sum(jnp.sum(acc[...], axis=1), axis=1, keepdims=True)
        each = jnp.broadcast_to(each, (count, BLK))
        for k in range(pairs):
            line = jnp.sum(jnp.where(index == place * pairs + k, each, 0.0), axis=0, keepdims=True)
            stat = jnp.where(which == 2 * k + p, jnp.broadcast_to(line, (height, BLK)), stat)
    gathered[me] = stat

    def give(i):
        return pltpu.make_async_remote_copy(
            src_ref=gathered.at[me],
            dst_ref=gathered.at[me],
            send_sem=r_send.at[i],
            recv_sem=r_recv.at[i],
            device_id=at(i),
            device_id_type=MESH,
        )

    order = sorted(range(1, n_tm), key=lambda i: -min(i, n_tm - i))
    for i in order:
        give(i).start()
    out_ref[0] = stat
    for n in range(stages):
        for j in range(n_mom - 1):
            across(n, j).wait_send()
    for i in range(steps):
        far(i, own).wait_send()
    for g in range(groups):
        for q in range(2, slots):
            near(q, g, own).wait_send()

    @pl.when(odd_chip)
    def _():
        for g in range(groups):
            near(1, g, own).wait_send()
        for i in detour:
            pass_early(i).wait_send()

    @pl.when(even_chip)
    def _():
        for g in range(groups):
            kept = [i for i in range(g * parts, (g + 1) * parts) if i not in detour]
            if len(kept) == parts:
                near(1, g, own).wait_send()
            else:
                for i in kept:
                    near_piece(i, own).wait_send()
        for i in detour:
            give_early(i).wait_send()

    for i in reversed(order):
        give(i).wait()
    out_ref[1] = jnp.sum(gathered[...], axis=0)


def split(stat_ref, local_ref, sum_ref):
    pairs, _, seps = local_ref.shape
    for ref, place in ((local_ref, 0), (sum_ref, 1)):
        for k in range(pairs):
            ref[k] = stat_ref[place, 2 * k : 2 * k + 2, :seps]


def per_device(n_tm, n_mom, fields, mom_pairs, deltas):
    _, per_group, _, nev, _ = fields.shape
    pairs = mom_pairs.shape[0]
    seps = deltas.shape[0]
    stages = nev // BLK
    slots = 4
    groups = nev // ROWS
    steps = groups * per_group * 2
    meetings = 2
    reach = 4
    while 2 * reach < n_tm:
        meetings += 1
        reach *= 2
    count = -(-slots * pairs // 8) * 8
    height = -(-2 * pairs // 8) * 8
    dma = pltpu.SemaphoreType.DMA
    scratch = (
        [pltpu.VMEM((n_mom * per_group, 2, nev, BLK), fields.dtype)] * stages
        + [pltpu.VMEM((per_group, 2, ROWS, nev), fields.dtype)] * (groups * (slots + 1))
        + [pltpu.VMEM((max(EARLY, 1), ROWS, nev), fields.dtype)]
        + [pltpu.VMEM((count, 8, BLK), jnp.float32)] * 2
        + [pltpu.VMEM((count, stages, 2, BLK, BLK), jnp.float32)]
        + [pltpu.VMEM((count, stages - 1, 2, ROWS, BLK), jnp.float32)]
        + [pltpu.VMEM((n_tm, height, BLK), jnp.float32)]
        + [dma((groups,)), dma((stages,))]
        + [dma((stages, n_mom))] * 2
        + [dma((steps,))] * 2
        + [dma((slots - 1, groups))] * 2
        + [dma((max(EARLY, 1),))] * 3
        + [dma((n_tm,))] * 2
        + [pltpu.SemaphoreType.REGULAR, pltpu.SemaphoreType.REGULAR((meetings,))]
    )
    stat = pl.pallas_call(
        functools.partial(kernel, n_tm, n_mom),
        out_shape=jax.ShapeDtypeStruct((2, height, BLK), jnp.float32),
        in_specs=[
            pl.BlockSpec(memory_space=pltpu.SMEM),
            pl.BlockSpec(memory_space=pltpu.SMEM),
            pl.BlockSpec(memory_space=pltpu.HBM),
        ],
        out_specs=pl.BlockSpec(memory_space=pltpu.VMEM),
        scratch_shapes=scratch,
        compiler_params=pltpu.CompilerParams(
            collective_id=0, has_side_effects=True, vmem_limit_bytes=67_043_328
        ),
    )(mom_pairs.T, deltas, fields)
    tile = jax.ShapeDtypeStruct((pairs, 2, seps), jnp.float32)
    local, total = pl.pallas_call(
        split,
        out_shape=(tile, tile),
        in_specs=[pl.BlockSpec(memory_space=pltpu.VMEM)],
        out_specs=(pl.BlockSpec(memory_space=pltpu.VMEM), pl.BlockSpec(memory_space=pltpu.VMEM)),
    )(stat)
    return (local.transpose(1, 2, 0)[None], total.transpose(1, 2, 0))


def solution(mesh):
    return jax.shard_map(
        functools.partial(per_device, mesh.shape["tm"], mesh.shape["mom"]),
        mesh=mesh,
        in_specs=(P("tm", "mom", None, None, None), P("mom", None), P()),
        out_specs=(P("tm", None, None, "mom"), P(None, None, "mom")),
        check_vma=False,
    )
```
